256 devices in a mesh: ctx: 32 (over z_lo, x, core), exp: 8 (over z_hi, y).
Axes of the slice: x: 4, y: 4, z: 8 (z_hi: 2, z_lo: 4; z = z_hi * 4 + z_lo), core: 2. Of those that a mesh axis runs over, the one named last changes fastest.
Arguments:
- hidden_in: bfloat16 [4096, 4096], P('ctx', 'exp'), may hold values from -6 to 6
- query_vectors: bfloat16 [4096, 2048], P('ctx', 'exp'), may hold values from -6 to 6
- key_vectors: bfloat16 [4096, 2048], P('ctx', 'exp'), may hold values from -6 to 6
- value_vectors: bfloat16 [4096, 2048], P('ctx', 'exp'), may hold values from -24 to 24
- out_weight: bfloat16 [2048, 4096], P('exp'), may hold values from -0.125 to 0.125
- norm_gain: float32 [4096], replicated, may hold values from 0.5 to 1.5
- gate_proj: bfloat16 [8, 4096, 11008], P('exp', None, 'ctx'), may hold values from -0.09375 to 0.09375
- up_proj: bfloat16 [8, 4096, 11008], P('exp', None, 'ctx'), may hold values from -0.09375 to 0.09375
- down_proj: bfloat16 [8, 11008, 4096], P('exp', 'ctx'), may hold values from -0.0546875 to 0.0546875
- expert_ids: int32 [4096, 2], P('ctx'), may hold values from 0 to 7, all different within a row; in each aligned block of 128 rows (0 to 127, 128 to 255, ...) at most 40 rows name the same one
- gate_scale: float32 [4096, 2], P('ctx'), may hold values from 0.1 to 1
Outputs:
- layer_out: bfloat16 [4096, 4096], P('ctx', 'exp')
The draws below stay inside these ranges and needn't reach their ends.
Inputs may be any that keep to these rules, and one draw needn't show every extreme that they name: `expert_ids`: each row names two different experts. In each aligned block of 128 rows (the rows of one ctx device) no expert is named by more than 40 rows, and in some blocks some expert is named by exactly 40 rows.
All inputs are finite; a program needn't handle non-finite values.
Results may differ from the reference program's by a relative error of at most 0.017.
Values may be sent and summed in bfloat16 or wider, within the bound.
No kernel may reach another device: no remote copies, remote signals or barrier semaphores. Data moves between devices by JAX's collectives and lax.ppermute only.
A program may use at most 128 MiB of HBM per device.

```python
import math
import jax
import jax.numpy as jnp
import numpy as np
from jax import lax

D = 4096
HEADS = 16
HEAD_DIM = 128
FF = 11008
TOK_DEV = 128
TOKENS = 4096
EXPERTS = 8
CAP = 40
N_CTX = 32


def draw_pair(key):
    shape = (TOKENS, HEADS * HEAD_DIM)
    first = jnp.clip(jax.random.normal(jax.random.fold_in(key, 11), shape, jnp.float32), -6.0, 6.0)
    second = jnp.clip(jax.random.normal(jax.random.fold_in(key, 12), shape, jnp.float32), -6.0, 6.0)
    return (first, second)


def draw_query_vectors(key, part):
    return draw_pair(key)[0].astype(jnp.bfloat16)


def draw_key_vectors(key, part):
    return draw_pair(key)[1].astype(jnp.bfloat16)


def draw_hidden_in(key, part):
    shape = (TOKENS, D)
    log_scale = jax.random.uniform(jax.random.fold_in(key, 21), (TOKENS, 1), jnp.float32, jnp.log(0.3), jnp.log(1.5))
    row_scale = jnp.exp(log_scale)
    fraction = jnp.arange(D, dtype=jnp.float32)[None, :] / (D - 1)
    column_scale = jnp.exp(jnp.log(0.4) + fraction * (jnp.log(2.0) - jnp.log(0.4)))
    entries = jax.random.normal(jax.random.fold_in(key, 22), shape, jnp.float32)
    return jnp.clip(entries * row_scale * column_scale, -6.0, 6.0).astype(jnp.bfloat16)


def shard_levels(stream_key, shape, shards, least, largest):
    def one(position, parts):
        draws = jax.random.uniform(jax.random.fold_in(jax.random.fold_in(stream_key, 6), position), (parts,), jnp.float32, least / len(shards), largest / len(shards))
        return jnp.repeat(jnp.exp(draws), shape[position] // parts).reshape((-1,) + (1,) * (len(shape) - position - 1))

    loudness = one(*shards[0])
    for cut in shards[1:]:
        loudness = loudness * one(*cut)
    return loudness


def assign_block(own_key, own, number, rows, count, top, most, lean):
    order = jax.random.permutation(own_key, count)
    heavy_load, ordinary = portions_of(count, rows * top, most, lean, True), portions_of(count, rows * top, most, lean, False)
    places = jnp.arange(count)

    def named(tallies, offset_by):
        used = int((tallies > 0).sum())
        fixed = max(1, used // 4)
        shifted = fixed + (places - fixed + offset_by * (used - fixed)) % max(1, count - fixed)
        return jnp.zeros((count,), jnp.int32).at[order[jnp.where(places < fixed, places, shifted)]].set(jnp.asarray(tallies, jnp.int32))

    tallies = jnp.where(number % 4 == 0, named(heavy_load, number // 4), named(ordinary, number - number // 4 - 1))
    mixed = jax.random.permutation(jax.random.fold_in(own, 3), count)
    donor, taker = mixed[0:count // 2 * 2:2], mixed[1:count // 2 * 2:2]
    slack = jnp.minimum(tallies[donor] - 1, most - tallies[taker]) // 2
    slack = jnp.where((donor == order[0]) | (taker == order[0]) | (tallies[taker] == 0), 0, jnp.maximum(slack, 0))
    shifted = jax.random.randint(jax.random.fold_in(own, 4), (count // 2,), 0, 1 << 20) % (slack + 1)
    tallies = tallies.at[donor].add(-shifted).at[taker].add(shifted)
    members = jnp.searchsorted(jnp.cumsum(tallies), jnp.arange(rows * top), side="right").astype(jnp.int32)
    grid = members.reshape(top, rows).T
    grid = grid[jax.random.permutation(jax.random.fold_in(own, 1), rows)]
    offset_by = jax.random.randint(jax.random.fold_in(own, 2), (rows, 1), 0, top)
    return jnp.take_along_axis(grid, (jnp.arange(top)[None, :] + offset_by) % top, axis=1)


def portions_of(number_of, total, limit, skew, full):
    weights = [(1 << 20) // math.isqrt(grade ** skew) + 1 for grade in range(1, number_of + 1)]
    largest = limit if full else min(limit, max(-(-total // number_of), total * weights[0] // sum(weights)))
    least = 1 if total - largest >= number_of - 1 else 0
    given, rest = [largest] + [least] * (number_of - 1), total - largest - least * (number_of - 1)
    while rest > 0:
        free = [i for i in range(1, number_of) if given[i] < largest] or [i for i in range(1, number_of) if given[i] < limit]
        whole, left = sum([weights[i] for i in free]), rest
        for i in free:
            extra = min(limit - given[i], max(1, left * weights[i] // whole), rest)
            given[i] = given[i] + extra
            rest = rest - extra
    return np.array(given)


def gaussian(rng, dims, width, bound, cuts=(), held_as=jnp.bfloat16):
    values = jax.random.normal(rng, dims, jnp.float32) * width
    if len(cuts) > 0:
        values = shard_levels(rng, dims, cuts, -0.22, 0.18) * values
    return jnp.clip(values, min=-bound, max=bound).astype(held_as)


def setup_inputs(seed: int = 0) -> dict:
    key_of = jax.random.split(jax.random.key(seed), 12)
    hidden_in = draw_hidden_in(jax.random.fold_in(key_of[11], 71), 0)
    query_vectors = draw_query_vectors(jax.random.fold_in(key_of[11], 71), 0)
    key_vectors = draw_key_vectors(jax.random.fold_in(key_of[11], 71), 0)
    value_vectors = gaussian(key_of[3], (TOKENS, HEADS * HEAD_DIM), 4.0, 24.0, ((0, 32), (1, 8)))
    out_weight = gaussian(key_of[4], (HEADS * HEAD_DIM, D), (HEADS * HEAD_DIM) ** -0.5, 0.125, ((0, 8),))
    norm_gain = jnp.clip(1.0 + 0.1 * jax.random.normal(key_of[5], (D,), jnp.float32), 0.5, 1.5)
    gate_proj = gaussian(key_of[6], (EXPERTS, D, FF), D ** -0.5, 0.09375, ((0, 8), (2, 32)))
    up_proj = gaussian(key_of[7], (EXPERTS, D, FF), D ** -0.5, 0.09375, ((0, 8), (2, 32)))
    down_proj = gaussian(key_of[8], (EXPERTS, FF, D), FF ** -0.5, 0.0546875, ((0, 8), (1, 32)))
    expert_ids_keys = jax.random.split(jax.random.fold_in(key_of[9], 1), TOKENS // TOK_DEV)
    expert_ids_turns = jax.random.permutation(jax.random.fold_in(key_of[9], 3), TOKENS // TOK_DEV)
    expert_ids = jax.vmap(lambda own, number: assign_block(jax.random.fold_in(key_of[9], 2), own, number, TOK_DEV, EXPERTS, 2, CAP, 2))(expert_ids_keys, expert_ids_turns).reshape((TOKENS, 2))
    gate_scale = jnp.clip(0.1 + 0.9 * jax.random.uniform(key_of[10], (TOKENS, 2), jnp.float32) ** shard_levels(key_of[10], (TOKENS, 2), ((0, 32),), -0.2, 0.2), 0.1, 1.0)
    return dict(hidden_in=hidden_in, query_vectors=query_vectors, key_vectors=key_vectors, value_vectors=value_vectors, out_weight=out_weight, norm_gain=norm_gain, gate_proj=gate_proj, up_proj=up_proj, down_proj=down_proj, expert_ids=expert_ids, gate_scale=gate_scale)


epsilon = 1e-05

def attend_head(query_head, key_head, value_head):
    scores = jnp.dot(query_head, key_head.T, preferred_element_type=jnp.float32) * HEAD_DIM ** (-0.5)
    row_pos = lax.broadcasted_iota(jnp.int32, scores.shape, 0)
    col_pos = lax.broadcasted_iota(jnp.int32, scores.shape, 1)
    visible = col_pos <= row_pos
    scores = jnp.where(visible, scores, -1e+30)
    row_max = lax.optimization_barrier(jnp.max(scores, axis=1, keepdims=True))
    weights = jnp.where(visible, jnp.exp(scores - row_max), 0.0)
    denominator = lax.optimization_barrier(jnp.sum(weights, axis=1, keepdims=True))
    head_out = jnp.dot(weights.astype(jnp.bfloat16), value_head, preferred_element_type=jnp.float32)
    return head_out / denominator

def reference(hidden_in, query_vectors, key_vectors, value_vectors, out_weight, norm_gain, gate_proj, up_proj, down_proj, expert_ids, gate_scale):
    query_split = query_vectors.reshape(TOKENS, HEADS, HEAD_DIM).transpose(1, 0, 2)
    key_split = key_vectors.reshape(TOKENS, HEADS, HEAD_DIM).transpose(1, 0, 2)
    value_split = value_vectors.reshape(TOKENS, HEADS, HEAD_DIM).transpose(1, 0, 2)
    attended = lax.map(lambda triple: attend_head(triple[0], triple[1], triple[2]), (query_split, key_split, value_split))
    attended = attended.transpose(1, 0, 2).reshape(TOKENS, HEADS * HEAD_DIM).astype(jnp.bfloat16)
    projected = jnp.dot(attended, out_weight, preferred_element_type=jnp.float32)
    residual = (hidden_in.astype(jnp.float32) + projected).astype(jnp.bfloat16)
    residual_wide = residual.astype(jnp.float32)
    inverse = lax.rsqrt(lax.optimization_barrier(jnp.mean(residual_wide * residual_wide, axis=1, keepdims=True)) + epsilon)
    normed = (residual_wide * inverse * norm_gain.astype(jnp.float32)[None, :]).astype(jnp.bfloat16)
    block_ids = expert_ids.reshape(N_CTX, TOK_DEV * 2)
    onehot = (block_ids[:, :, None] == jnp.arange(EXPERTS, dtype=jnp.int32)[None, None, :]).astype(jnp.int32)
    earlier = jnp.cumsum(onehot, axis=1) - onehot
    slot_index = lax.optimization_barrier(jnp.sum(earlier * onehot, axis=2))
    slot_row = (jnp.arange(N_CTX, dtype=jnp.int32)[:, None] * CAP + slot_index).reshape(-1).astype(jnp.int32)
    flat_ids = expert_ids.reshape(-1)
    source = jnp.repeat(normed, 2, axis=0)
    rows_all = N_CTX * CAP
    group_width = FF // N_CTX

    def per_expert(running, expert_index):
        target = jnp.where(flat_ids == expert_index, slot_row, rows_all).astype(jnp.int32)
        buffer = jnp.zeros((rows_all, D), jnp.bfloat16).at[target].set(source, mode='drop')
        gate_act = jnp.dot(buffer, gate_proj[expert_index], preferred_element_type=jnp.float32)
        up_act = jnp.dot(buffer, up_proj[expert_index], preferred_element_type=jnp.float32)
        hidden = (jax.nn.silu(gate_act) * up_act).astype(jnp.bfloat16)
        down_one = down_proj[expert_index]

        def add_group(group_index, summed):
            piece_in = lax.dynamic_slice_in_dim(hidden, group_index * group_width, group_width, 1)
            piece_weight = lax.dynamic_slice_in_dim(down_one, group_index * group_width, group_width, 0)
            piece_out = jnp.dot(piece_in, piece_weight, preferred_element_type=jnp.float32).astype(jnp.bfloat16)
            piece_out = lax.optimization_barrier(piece_out)
            return summed + piece_out.astype(jnp.float32)
        expert_out = lax.fori_loop(0, N_CTX, add_group, jnp.zeros((rows_all, D), jnp.float32)).astype(jnp.bfloat16)
        picked = expert_out[jnp.clip(slot_row, 0, rows_all - 1)]
        running = running + jnp.where((flat_ids == expert_index)[:, None], picked.astype(jnp.float32), 0.0)
        return (running, None)
    gathered, _ = lax.scan(per_expert, jnp.zeros((TOKENS * 2, D), jnp.float32), jnp.arange(EXPERTS, dtype=jnp.int32))
    gathered = gathered.reshape(TOKENS, 2, D)
    layer_out = residual_wide + gate_scale[:, 0:1] * gathered[:, 0] + gate_scale[:, 1:2] * gathered[:, 1]
    return layer_out.astype(jnp.bfloat16)
```

```python
import functools

import jax
import jax.numpy as jnp
from jax import lax
from jax.experimental import pallas as pl
from jax.experimental.pallas import tpu as pltpu
from jax.sharding import Mesh
from jax.sharding import PartitionSpec as P

HEAD_DIM = 128
EPSILON = 1e-05
MASKED = -1e30

AXES = ("zlo", "x", "core", "zhi", "y")
CTX = ("zlo", "x", "core")
RING = ("zlo", "x")
EXP = ("zhi", "y")
SWAP = [(0, 1), (1, 0)]

NT = (((1,), (1,)), ((), ()))


def attention_kernel(
    block_ref, query_ref, kv_ref, out_ref, max_ref, sum_ref, acc_ref, *, heads, chunk
):
    step = pl.program_id(0)
    rows = query_ref.shape[0]
    start = block_ref[0] * rows

    @pl.when(step == 0)
    def _():
        max_ref[...] = jnp.full_like(max_ref, MASKED)
        sum_ref[...] = jnp.zeros_like(sum_ref)
        acc_ref[...] = jnp.zeros_like(acc_ref)

    @pl.when(step * chunk < start + rows)
    def _():
        query_pos = start + lax.broadcasted_iota(jnp.int32, (rows, chunk), 0)
        key_pos = step * chunk + lax.broadcasted_iota(jnp.int32, (rows, chunk), 1)
        visible = key_pos <= query_pos
        for h in range(heads):
            cols = slice(h * HEAD_DIM, (h + 1) * HEAD_DIM)
            value_cols = slice((heads + h) * HEAD_DIM, (heads + h + 1) * HEAD_DIM)
            scores = lax.dot_general(
                query_ref[:, cols], kv_ref[:, cols], NT, preferred_element_type=jnp.float32
            ) * HEAD_DIM ** (-0.5)
            scores = jnp.where(visible, scores, MASKED)
            old_max = max_ref[h]
            new_max = jnp.maximum(old_max, jnp.max(scores, axis=1, keepdims=True))
            weights = jnp.where(visible, jnp.exp(scores - new_max[:, :1]), 0.0)
            rescale = jnp.exp(old_max - new_max)
            max_ref[h] = new_max
            sum_ref[h] = sum_ref[h] * rescale + jnp.sum(weights, axis=1, keepdims=True)
            acc_ref[h] = acc_ref[h] * rescale + jnp.dot(
                weights.astype(jnp.bfloat16),
                kv_ref[:, value_cols],
                preferred_element_type=jnp.float32,
            )

    @pl.when(step == pl.num_programs(0) - 1)
    def _():
        for h in range(heads):
            out_ref[:, h * HEAD_DIM : (h + 1) * HEAD_DIM] = (acc_ref[h] / sum_ref[h]).astype(
                out_ref.dtype
            )


def attention(block, query, kv, chunk=512):
    rows, width = query.shape
    heads = width // HEAD_DIM
    keys = kv.shape[0]

    def kv_index(step, block_ref):
        return (jnp.minimum(step, ((block_ref[0] + 1) * rows - 1) // chunk), 0)

    return pl.pallas_call(
        functools.partial(attention_kernel, heads=heads, chunk=chunk),
        grid_spec=pltpu.PrefetchScalarGridSpec(
            num_scalar_prefetch=1,
            grid=(keys // chunk,),
            in_specs=[
                pl.BlockSpec((rows, width), lambda step, block_ref: (0, 0)),
                pl.BlockSpec((chunk, 2 * width), kv_index),
            ],
            out_specs=pl.BlockSpec((rows, width), lambda step, block_ref: (0, 0)),
            scratch_shapes=[
                pltpu.VMEM((heads, rows, HEAD_DIM), jnp.float32),
                pltpu.VMEM((heads, rows, HEAD_DIM), jnp.float32),
                pltpu.VMEM((heads, rows, HEAD_DIM), jnp.float32),
            ],
        ),
        out_shape=jax.ShapeDtypeStruct((rows, width), jnp.bfloat16),
        cost_estimate=pl.CostEstimate(
            flops=4 * rows * width * keys,
            bytes_accessed=4 * keys * width,
            transcendentals=heads * rows * keys,
        ),
    )(block, query, kv)


def local(
    hidden_in,
    query_vectors,
    key_vectors,
    value_vectors,
    out_weight,
    norm_gain,
    gate_proj,
    up_proj,
    down_proj,
    expert_ids,
    gate_scale,
):
    row_count, local_width = hidden_in.shape
    model_width = out_weight.shape[1]
    expert_count = lax.axis_size(EXP)
    capacity = min(row_count, 5 * row_count // (2 * expert_count))

    kv = lax.all_gather(
        jnp.concatenate([key_vectors, value_vectors], axis=1), CTX, axis=0, tiled=True
    )

    def doubled(own):
        other = lax.ppermute(own, "core", SWAP)
        pad = jnp.zeros((-2 * own.shape[0] % 256, own.shape[1]), own.dtype)
        return jnp.concatenate([own, other, pad], axis=0)

    w_in = jnp.concatenate([doubled(gate_proj[0].T), doubled(up_proj[0].T)], axis=0)
    w_down = doubled(down_proj[0])
    units = w_down.shape[0]

    flat_ids = expert_ids.reshape(row_count * 2)
    onehot = (
        flat_ids[:, None] == lax.broadcasted_iota(jnp.int32, (row_count * 2, expert_count), 1)
    ).astype(jnp.int32)
    earlier = jnp.cumsum(onehot, axis=0) - onehot
    slot_index = jnp.sum(earlier * onehot, axis=1)
    target = flat_ids * capacity + slot_index
    placing = (
        target[None, :]
        == lax.broadcasted_iota(jnp.int32, (expert_count * capacity, row_count * 2), 0)
    ).astype(jnp.bfloat16)
    placing_tokens = jnp.sum(placing.reshape(expert_count * capacity, row_count, 2), axis=2)

    w_out = lax.all_to_all(out_weight, EXP, split_axis=1, concat_axis=0, tiled=True)

    block = lax.axis_index(CTX).reshape(1)
    attended = attention(block, query_vectors, kv)
    all_heads = lax.all_gather(attended, EXP, axis=1, tiled=True)
    projected = jnp.dot(all_heads, w_out, preferred_element_type=jnp.float32)
    residual = (hidden_in.astype(jnp.float32) + projected).astype(jnp.bfloat16)
    residual_wide = residual.astype(jnp.float32)

    buffer = jnp.dot(placing_tokens, residual, preferred_element_type=jnp.float32).astype(
        jnp.bfloat16
    )
    arrived = lax.all_to_all(buffer, EXP, split_axis=0, concat_axis=1, tiled=True)
    arrived_wide = arrived.astype(jnp.float32)
    inverse = lax.rsqrt(jnp.mean(arrived_wide * arrived_wide, axis=1, keepdims=True) + EPSILON)
    normed = (arrived_wide * inverse * norm_gain[None, :]).astype(jnp.bfloat16)

    rows = lax.all_gather(normed, RING, axis=0, tiled=True)
    act = lax.dot_general(rows, w_in, NT, preferred_element_type=jnp.float32)
    hidden = (jax.nn.silu(act[:, :units]) * act[:, units:]).astype(jnp.bfloat16)
    result = lax.psum_scatter(
        jnp.dot(hidden, w_down, preferred_element_type=jnp.float32).astype(jnp.bfloat16),
        RING,
        scatter_dimension=0,
        tiled=True,
    )
    returned = lax.all_to_all(result, EXP, split_axis=1, concat_axis=0, tiled=True)
    gathered_back = lax.dot_general(
        placing, returned, (((0,), (0,)), ((), ())), preferred_element_type=jnp.float32
    )
    gathered_back = gathered_back.reshape(row_count, 2, local_width)
    combined = (
        residual_wide
        + gate_scale[:, 0:1] * gathered_back[:, 0]
        + gate_scale[:, 1:2] * gathered_back[:, 1]
    )
    return combined.astype(jnp.bfloat16)


def solution(mesh):
    fine = Mesh(mesh.devices.reshape(4, 4, 2, 2, 4), AXES)
    placed = (
        P(CTX, EXP),
        P(CTX, EXP),
        P(CTX, EXP),
        P(CTX, EXP),
        P(EXP, None),
        P(),
        P(EXP, None, CTX),
        P(EXP, None, CTX),
        P(EXP, CTX, None),
        P(CTX, None),
        P(CTX, None),
    )
    return jax.shard_map(
        local, mesh=fine, in_specs=placed, out_specs=P(CTX, EXP), check_vma=False
    )
```

```python
import functools

import jax
import jax.numpy as jnp
from jax import lax
from jax.experimental import pallas as pl
from jax.experimental.pallas import tpu as pltpu
from jax.sharding import Mesh
from jax.sharding import PartitionSpec as P

HEAD_DIM = 128
EPSILON = 1e-05
MASKED = -1e30

AXES = ("zlo", "x", "core", "zhi", "y")
CTX = ("zlo", "x", "core")
RING = ("zlo", "x")
EXP = ("zhi", "y")
SWAP = [(0, 1), (1, 0)]

NT = (((1,), (1,)), ((), ()))


def attention_kernel(
    order_ref, query_ref, query_pos_ref, key_pos_ref, weight_ref, *refs, heads, chunk
):
    kv_refs, (out_ref, scores_ref, attended_ref) = refs[:-3], refs[-3:]
    rows = query_ref.shape[0]
    query_pos = query_pos_ref[...]
    chunks = [(ref, start) for ref in kv_refs for start in range(0, ref.shape[0], chunk)]
    for h in range(heads):
        cols = slice(h * HEAD_DIM, (h + 1) * HEAD_DIM)
        value_cols = slice((heads + h) * HEAD_DIM, (heads + h + 1) * HEAD_DIM)
        query = query_ref[:, cols]
        largest = jnp.full((rows, 128), MASKED, jnp.float32)
        for c, (ref, start) in enumerate(chunks):
            at = slice(c * chunk, (c + 1) * chunk)
            scores = lax.dot_general(
                query, ref[start : start + chunk, cols], NT, preferred_element_type=jnp.float32
            ) * HEAD_DIM ** (-0.5)
            scores = jnp.where(key_pos_ref[:, at] <= query_pos, scores, MASKED)
            scores_ref[:, at] = scores
            for lane in range(0, chunk, 128):
                largest = jnp.maximum(largest, scores[:, lane : lane + 128])
        largest = jnp.max(largest, axis=1, keepdims=True)
        total = jnp.zeros((rows, 128), jnp.float32)
        acc = jnp.zeros((rows, HEAD_DIM), jnp.float32)
        for c, (ref, start) in enumerate(chunks):
            weights = jnp.exp(scores_ref[:, c * chunk : (c + 1) * chunk] - largest)
            for lane in range(0, chunk, 128):
                total = total + weights[:, lane : lane + 128]
            acc = acc + jnp.dot(
                weights.astype(jnp.bfloat16),
                ref[start : start + chunk, value_cols],
                preferred_element_type=jnp.float32,
            )
        attended_ref[:, cols] = (acc / jnp.sum(total, axis=1, keepdims=True)).astype(
            attended_ref.dtype
        )
    parts = order_ref.shape[0]
    width = weight_ref.shape[1] // parts
    for j in range(parts):
        start = pl.multiple_of(order_ref[j] * width, width)
        out_ref[:, j * width : (j + 1) * width] = jnp.dot(
            attended_ref[...],
            weight_ref[:, pl.ds(start, width)],
            preferred_element_type=jnp.float32,
        )


def attention(query, query_pos, key_pos, kv, weight, order, chunk=512):
    rows, width = query.shape
    heads = width // HEAD_DIM
    keys = sum(part.shape[0] for part in kv)
    vmem = pl.BlockSpec(memory_space=pltpu.VMEM)
    return pl.pallas_call(
        functools.partial(attention_kernel, heads=heads, chunk=chunk),
        in_specs=[pl.BlockSpec(memory_space=pltpu.SMEM)] + [vmem] * (4 + len(kv)),
        out_specs=vmem,
        scratch_shapes=[
            pltpu.VMEM((rows, keys), jnp.float32),
            pltpu.VMEM((rows, width), jnp.bfloat16),
        ],
        out_shape=jax.ShapeDtypeStruct((rows, weight.shape[1]), jnp.float32),
        cost_estimate=pl.CostEstimate(
            flops=4 * rows * width * keys + 2 * rows * weight.size,
            bytes_accessed=4 * keys * width,
            transcendentals=heads * rows * keys,
        ),
    )(order, query, query_pos, key_pos, weight, *kv)


UNIT_TILE = 256


def expert_kernel(
    rows_ref, gate, gate_too, up, up_too, down, down_too, out_ref, w_in, w_down, hidden_ref, sems
):
    share = gate.shape[0]
    units = w_down.shape[0]
    half = units // 2
    copies = []
    for i, (source, target, start) in enumerate(
        [
            (gate, w_in, 0),
            (up, w_in, units),
            (gate_too, w_in, half),
            (up_too, w_in, units + half),
            (down, w_down, 0),
            (down_too, w_down, half),
        ]
    ):
        copy = pltpu.make_async_copy(source, target.at[pl.ds(start, share)], sems.at[i])
        copy.start()
        copies.append(copy)
    for target in (w_in, w_down):
        for start in range(0, target.shape[0], half):
            target[start + share : start + half] = jnp.zeros(
                (half - share, target.shape[1]), target.dtype
            )
    rows = rows_ref[...]
    ready = 0
    for start in range(0, units, UNIT_TILE):
        needed = 2 if start + UNIT_TILE <= half else 4
        while ready < needed:
            copies[ready].wait()
            ready += 1
        gate_act = lax.dot_general(
            rows, w_in[start : start + UNIT_TILE], NT, preferred_element_type=jnp.float32
        )
        up_act = lax.dot_general(
            rows,
            w_in[units + start : units + start + UNIT_TILE],
            NT,
            preferred_element_type=jnp.float32,
        )
        hidden_ref[:, start : start + UNIT_TILE] = (
            gate_act / (1.0 + jnp.exp(-gate_act)) * up_act
        ).astype(hidden_ref.dtype)
    for copy in copies[ready:]:
        copy.wait()
    hidden = hidden_ref[...]
    width = w_down.shape[1]
    for start in range(0, width, 512):
        out_ref[:, start : start + 512] = jnp.dot(
            hidden, w_down[:, start : start + 512], preferred_element_type=jnp.float32
        ).astype(out_ref.dtype)


def expert(rows, weights):
    count, width = rows.shape
    share = weights[0].shape[0]
    units = 2 * (-(-share // 128) * 128)
    return pl.pallas_call(
        expert_kernel,
        in_specs=[pl.BlockSpec(memory_space=pltpu.VMEM)]
        + [pl.BlockSpec(memory_space=pltpu.HBM)] * len(weights),
        out_specs=pl.BlockSpec(memory_space=pltpu.VMEM),
        scratch_shapes=[
            pltpu.VMEM((2 * units, width), jnp.bfloat16),
            pltpu.VMEM((units, width), jnp.bfloat16),
            pltpu.VMEM((count, units), jnp.bfloat16),
            pltpu.SemaphoreType.DMA((6,)),
        ],
        out_shape=jax.ShapeDtypeStruct((count, width), jnp.bfloat16),
        cost_estimate=pl.CostEstimate(
            flops=12 * count * width * share,
            bytes_accessed=12 * share * width,
            transcendentals=2 * count * share,
        ),
        compiler_params=pltpu.CompilerParams(vmem_limit_bytes=44 * 1024 * 1024),
    )(rows, *weights)


def hop(v, axis, step):
    n = lax.axis_size(axis)
    return lax.ppermute(v, axis, [(i, (i + step) % n) for i in range(n)])


def first_part(v):
    return (v.shape[0] // 2 + 7) // 8 * 8


def plus(a, b):
    return a.astype(jnp.float32) + b.astype(jnp.float32)


def gather_ring(v, axis):
    cut = first_part(v)
    left = hop(v, axis, 1)
    right = hop(v, axis, -1)
    return [v, left, right, hop(left[:cut], axis, 1), hop(right[cut:], axis, -1)]


def reduce_ring(parts, axis):
    own, left, right, far_low, far_high = parts
    cut = far_low.shape[0]
    low = hop(far_low.astype(jnp.bfloat16), axis, -1)
    high = hop(far_high.astype(jnp.bfloat16), axis, 1)
    left = jnp.concatenate([plus(left[:cut], low).astype(jnp.bfloat16), left[cut:].astype(jnp.bfloat16)])
    right = jnp.concatenate([right[:cut].astype(jnp.bfloat16), plus(right[cut:], high).astype(jnp.bfloat16)])
    return plus(own, hop(left, axis, -1)) + hop(right, axis, 1).astype(jnp.float32)


def gather_across(v, axis):
    return [v, hop(v, axis, 1), hop(v, axis, -1), hop(v, axis, 2)]


def gather_before(v, axis):
    return [hop(v, axis, back) for back in (1, 2, 3)]


def send_back(parts, axis):
    return [hop(part, axis, -back) for back, part in zip((1, 2, 3), parts, strict=True)]


def gather_group(v, main):
    column = gather_before(v[:main], "zlo")
    near = gather_across(v, "x")
    far = gather_across(jnp.concatenate(column), "x")
    side = jnp.concatenate([part[main:] for part in near])
    return near, far + gather_before(side, "zlo")


def positions_of(rows, main):
    z, x, core = (lax.axis_index(a) for a in ("zlo", "x", "core"))
    n_z, n_x, n_core = (lax.axis_size(a) for a in ("zlo", "x", "core"))

    def at(back, over, start, stop):
        block = ((z + n_z - back) % n_z * n_x + (x + n_x + over) % n_x) * n_core + core
        return block * rows + jnp.arange(start, stop, dtype=jnp.int32)

    near = [at(0, over, 0, rows) for over in (0, -1, 1, 2)]
    far = [at(back, over, 0, main) for over in (0, -1, 1, 2) for back in (1, 2, 3)]
    side = [at(back, over, main, rows) for back in (1, 2, 3) for over in (0, -1, 1, 2)]
    return jnp.concatenate(near), jnp.concatenate(far + side)


def pieces_of(v, sizes):
    out, start = [], 0
    for size in sizes:
        out.append(v[start : start + size])
        start += size
    return out


def routed_experts(normed, ffn):
    rows = normed.shape[0]
    main = rows * 4 // 5 // 8 * 8
    cut = first_part(normed)

    def side_of(ring):
        return [ring[0][main:], ring[1][main:], ring[2][main:], ring[4][main - cut :]]

    column = jnp.concatenate(gather_before(normed[:main], "zlo"))
    near = gather_ring(normed, "x")
    far = gather_ring(column, "x")
    far = far + gather_before(jnp.concatenate(side_of(near)), "zlo")
    near_rows, _ = lax.optimization_barrier((jnp.concatenate(near), column))
    near = pieces_of(ffn(near_rows), [p.shape[0] for p in near])
    far = pieces_of(ffn(jnp.concatenate(far)), [p.shape[0] for p in far])

    column = reduce_ring(far[:5], "x").astype(jnp.bfloat16)
    arrived = [v.astype(jnp.float32) for v in send_back(far[5:], "zlo")]
    side = jnp.concatenate(side_of(near)).astype(jnp.float32) + arrived[0] + arrived[1] + arrived[2]
    side = pieces_of(side.astype(jnp.bfloat16), [rows - main] * 4)
    near = [
        jnp.concatenate([near[0][:main], side[0]]),
        jnp.concatenate([near[1][:main], side[1]]),
        jnp.concatenate([near[2][:main], side[2]]),
        near[3],
        jnp.concatenate([near[4][: main - cut], side[3]]),
    ]
    near = reduce_ring(near, "x")
    arrived = [v.astype(jnp.float32) for v in send_back(pieces_of(column, [main] * 3), "zlo")]
    top = near[:main] + arrived[0] + arrived[1] + arrived[2]
    return jnp.concatenate([top, near[main:]]).astype(jnp.bfloat16)


def local(
    hidden_in,
    query_vectors,
    key_vectors,
    value_vectors,
    out_weight,
    norm_gain,
    gate_proj,
    up_proj,
    down_proj,
    expert_ids,
    gate_scale,
):
    row_count, local_width = hidden_in.shape
    expert_count = lax.axis_size(EXP)
    block = lax.axis_index(CTX)
    capacity = min(row_count, 5 * row_count // (2 * expert_count))

    kv_main = row_count * 4 // 5 // 32 * 32
    near, far = gather_group(jnp.concatenate([key_vectors, value_vectors], axis=1), kv_main)
    kv_near, kv_far = jnp.concatenate(near), jnp.concatenate(far)
    near_pos, far_pos = positions_of(row_count, kv_main)
    across = (1 - 2 * lax.axis_index("core")) * row_count
    key_pos = jnp.concatenate([near_pos, near_pos + across, far_pos, far_pos + across])[None, :]
    query_pos = (block * row_count + jnp.arange(row_count, dtype=jnp.int32))[:, None]
    kv = [kv_near, lax.ppermute(kv_near, "core", SWAP), kv_far, lax.ppermute(kv_far, "core", SWAP)]

    experts = []
    for own in (gate_proj[0].T, up_proj[0].T, down_proj[0]):
        experts += [own, lax.ppermute(own, "core", SWAP)]

    flat_ids = expert_ids.reshape(row_count * 2)
    onehot = (
        flat_ids[:, None] == lax.broadcasted_iota(jnp.int32, (row_count * 2, expert_count), 1)
    ).astype(jnp.int32)
    earlier = jnp.cumsum(onehot, axis=0) - onehot
    slot_index = jnp.sum(earlier * onehot, axis=1)
    target = flat_ids * capacity + slot_index
    placing = (
        target[None, :]
        == lax.broadcasted_iota(jnp.int32, (expert_count * capacity, row_count * 2), 0)
    ).astype(jnp.bfloat16)
    placing_tokens = jnp.sum(placing.reshape(expert_count * capacity, row_count, 2), axis=2)

    zhi, y = lax.axis_index("zhi"), lax.axis_index("y")
    n_zhi, n_y = lax.axis_size("zhi"), lax.axis_size("y")
    order = jnp.stack(
        [
            (zhi + a) % n_zhi * n_y + (y + n_y + b) % n_y
            for b in (0, -1, 1, 2)
            for a in range(n_zhi)
        ]
    ).astype(jnp.int32)
    kv, experts = lax.optimization_barrier((kv, experts))
    partial = attention(query_vectors, query_pos, key_pos, kv, out_weight, order)
    own, left, right, far = jnp.split(partial, 4, axis=1)
    cut = first_part(far)
    summed = reduce_ring([own, left, right, far[:cut], far[cut:]], "y")
    mine, theirs = jnp.split(summed, 2, axis=1)
    projected = plus(mine, lax.ppermute(theirs.astype(jnp.bfloat16), "zhi", SWAP))
    residual = (hidden_in.astype(jnp.float32) + projected).astype(jnp.bfloat16)
    residual_wide = residual.astype(jnp.float32)

    buffer = jnp.dot(placing_tokens, residual, preferred_element_type=jnp.float32).astype(
        jnp.bfloat16
    )
    arrived = lax.all_to_all(buffer, EXP, split_axis=0, concat_axis=1, tiled=True)
    arrived_wide = arrived.astype(jnp.float32)
    inverse = lax.rsqrt(jnp.mean(arrived_wide * arrived_wide, axis=1, keepdims=True) + EPSILON)
    normed = (arrived_wide * inverse * norm_gain[None, :]).astype(jnp.bfloat16)

    result = routed_experts(normed, lambda rows: expert(rows, experts))

    returned = lax.all_to_all(result, EXP, split_axis=1, concat_axis=0, tiled=True)
    gathered_back = lax.dot_general(
        placing, returned, (((0,), (0,)), ((), ())), preferred_element_type=jnp.float32
    )
    gathered_back = gathered_back.reshape(row_count, 2, local_width)
    combined = (
        residual_wide
        + gate_scale[:, 0:1] * gathered_back[:, 0]
        + gate_scale[:, 1:2] * gathered_back[:, 1]
    )
    return combined.astype(jnp.bfloat16)


def solution(mesh):
    fine = Mesh(mesh.devices.reshape(4, 4, 2, 2, 4), AXES)
    placed = (
        P(CTX, EXP),
        P(CTX, EXP),
        P(CTX, EXP),
        P(CTX, EXP),
        P(EXP, None),
        P(),
        P(EXP, None, CTX),
        P(EXP, None, CTX),
        P(EXP, CTX, None),
        P(CTX, None),
        P(CTX, None),
    )
    return jax.shard_map(
        local, mesh=fine, in_specs=placed, out_specs=P(CTX, EXP), check_vma=False
    )
```

```python
import functools

import jax
import jax.numpy as jnp
from jax import lax
from jax.experimental import pallas as pl
from jax.experimental.pallas import tpu as pltpu
from jax.sharding import Mesh
from jax.sharding import PartitionSpec as P

HEAD_DIM = 128
EPSILON = 1e-05
MASKED = -1e30

AXES = ("zlo", "x", "core", "zhi", "y")
CTX = ("zlo", "x", "core")
RING = ("zlo", "x")
EXP = ("zhi", "y")
SWAP = [(0, 1), (1, 0)]

NT = (((1,), (1,)), ((), ()))


def attention_kernel(
    order_ref, query_ref, query_pos_ref, key_pos_ref, weight_ref, *refs, heads, chunk
):
    kv_refs, out_refs, (scores_ref, attended_ref) = refs[:-6], refs[-6:-2], refs[-2:]
    rows = query_ref.shape[0]
    query_pos = query_pos_ref[...]
    chunks = [(ref, start) for ref in kv_refs for start in range(0, ref.shape[0], chunk)]
    for h in range(heads):
        cols = slice(h * HEAD_DIM, (h + 1) * HEAD_DIM)
        value_cols = slice((heads + h) * HEAD_DIM, (heads + h + 1) * HEAD_DIM)
        query = query_ref[:, cols]
        largest = jnp.full((rows, 128), MASKED, jnp.float32)
        for c, (ref, start) in enumerate(chunks):
            at = slice(c * chunk, (c + 1) * chunk)
            scores = lax.dot_general(
                query, ref[start : start + chunk, cols], NT, preferred_element_type=jnp.float32
            ) * HEAD_DIM ** (-0.5)
            scores = jnp.where(key_pos_ref[:, at] <= query_pos, scores, MASKED)
            scores_ref[:, at] = scores
            for lane in range(0, chunk, 128):
                largest = jnp.maximum(largest, scores[:, lane : lane + 128])
        largest = jnp.max(largest, axis=1, keepdims=True)
        total = jnp.zeros((rows, 128), jnp.float32)
        acc = jnp.zeros((rows, HEAD_DIM), jnp.float32)
        for c, (ref, start) in enumerate(chunks):
            weights = jnp.exp(scores_ref[:, c * chunk : (c + 1) * chunk] - largest)
            for lane in range(0, chunk, 128):
                total = total + weights[:, lane : lane + 128]
            acc = acc + jnp.dot(
                weights.astype(jnp.bfloat16),
                ref[start : start + chunk, value_cols],
                preferred_element_type=jnp.float32,
            )
        attended_ref[:, cols] = (acc / jnp.sum(total, axis=1, keepdims=True)).astype(
            attended_ref.dtype
        )
    width = weight_ref.shape[1] // order_ref.shape[0]
    per_out = order_ref.shape[0] // len(out_refs)
    for j in range(order_ref.shape[0]):
        start = pl.multiple_of(order_ref[j] * width, width)
        out_ref, at = out_refs[j // per_out], j % per_out * width
        out_ref[:, at : at + width] = jnp.dot(
            attended_ref[...],
            weight_ref[:, pl.ds(start, width)],
            preferred_element_type=jnp.float32,
        ).astype(out_ref.dtype)


def attention(query, query_pos, key_pos, kv, weight, order, chunk=512):
    rows, width = query.shape
    heads = width // HEAD_DIM
    keys = sum(part.shape[0] for part in kv)
    vmem = pl.BlockSpec(memory_space=pltpu.VMEM)
    return pl.pallas_call(
        functools.partial(attention_kernel, heads=heads, chunk=chunk),
        in_specs=[pl.BlockSpec(memory_space=pltpu.SMEM)] + [vmem] * (4 + len(kv)),
        out_specs=[vmem] * 4,
        scratch_shapes=[
            pltpu.VMEM((rows, keys), jnp.float32),
            pltpu.VMEM((rows, width), jnp.bfloat16),
        ],
        out_shape=[
            jax.ShapeDtypeStruct((rows, weight.shape[1] // 4), dtype)
            for dtype in (jnp.float32, jnp.bfloat16, jnp.bfloat16, jnp.bfloat16)
        ],
        cost_estimate=pl.CostEstimate(
            flops=4 * rows * width * keys + 2 * rows * weight.size,
            bytes_accessed=4 * keys * width,
            transcendentals=heads * rows * keys,
        ),
    )(order, query, query_pos, key_pos, weight, *kv)


UNIT_TILE = 256


def expert_kernel(
    rows_ref, gate, gate_too, up, up_too, down, down_too, out_ref, w_in, w_down, hidden_ref, sems
):
    share = gate.shape[0]
    units = w_down.shape[0]
    half = units // 2
    copies = []
    for i, (source, target, start) in enumerate(
        [
            (gate, w_in, 0),
            (up, w_in, units),
            (gate_too, w_in, half),
            (up_too, w_in, units + half),
            (down, w_down, 0),
            (down_too, w_down, half),
        ]
    ):
        copy = pltpu.make_async_copy(source, target.at[pl.ds(start, share)], sems.at[i])
        copy.start()
        copies.append(copy)
    for target in (w_in, w_down):
        for start in range(0, target.shape[0], half):
            target[start + share : start + half] = jnp.zeros(
                (half - share, target.shape[1]), target.dtype
            )
    rows = rows_ref[...]
    ready = 0
    for start in range(0, units, UNIT_TILE):
        needed = 2 if start + UNIT_TILE <= half else 4
        while ready < needed:
            copies[ready].wait()
            ready += 1
        gate_act = lax.dot_general(
            rows, w_in[start : start + UNIT_TILE], NT, preferred_element_type=jnp.float32
        )
        up_act = lax.dot_general(
            rows,
            w_in[units + start : units + start + UNIT_TILE],
            NT,
            preferred_element_type=jnp.float32,
        )
        hidden_ref[:, start : start + UNIT_TILE] = (
            gate_act / (1.0 + jnp.exp(-gate_act)) * up_act
        ).astype(hidden_ref.dtype)
    for copy in copies[ready:]:
        copy.wait()
    hidden = hidden_ref[...]
    width = w_down.shape[1]
    for start in range(0, width, 512):
        out_ref[:, start : start + 512] = jnp.dot(
            hidden, w_down[:, start : start + 512], preferred_element_type=jnp.float32
        ).astype(out_ref.dtype)


def expert(rows, weights):
    count, width = rows.shape
    share = weights[0].shape[0]
    units = 2 * (-(-share // 128) * 128)
    return pl.pallas_call(
        expert_kernel,
        in_specs=[pl.BlockSpec(memory_space=pltpu.VMEM)]
        + [pl.BlockSpec(memory_space=pltpu.HBM)] * len(weights),
        out_specs=pl.BlockSpec(memory_space=pltpu.VMEM),
        scratch_shapes=[
            pltpu.VMEM((2 * units, width), jnp.bfloat16),
            pltpu.VMEM((units, width), jnp.bfloat16),
            pltpu.VMEM((count, units), jnp.bfloat16),
            pltpu.SemaphoreType.DMA((6,)),
        ],
        out_shape=jax.ShapeDtypeStruct((count, width), jnp.bfloat16),
        cost_estimate=pl.CostEstimate(
            flops=12 * count * width * share,
            bytes_accessed=12 * share * width,
            transcendentals=2 * count * share,
        ),
        compiler_params=pltpu.CompilerParams(vmem_limit_bytes=44 * 1024 * 1024),
    )(rows, *weights)


def hop(v, axis, step):
    n = lax.axis_size(axis)
    return lax.ppermute(v, axis, [(i, (i + step) % n) for i in range(n)])


def first_part(v):
    return (v.shape[0] // 2 + 7) // 8 * 8


def plus(a, b):
    return a.astype(jnp.float32) + b.astype(jnp.float32)


def gather_ring(v, axis):
    cut = first_part(v)
    left = hop(v, axis, 1)
    right = hop(v, axis, -1)
    return [v, left, right, hop(left[:cut], axis, 1), hop(right[cut:], axis, -1)]


def reduce_ring(parts, axis):
    own, left, right, far_low, far_high = parts
    cut = far_low.shape[0]
    low = hop(far_low.astype(jnp.bfloat16), axis, -1)
    high = hop(far_high.astype(jnp.bfloat16), axis, 1)
    left = jnp.concatenate([plus(left[:cut], low).astype(jnp.bfloat16), left[cut:].astype(jnp.bfloat16)])
    right = jnp.concatenate([right[:cut].astype(jnp.bfloat16), plus(right[cut:], high).astype(jnp.bfloat16)])
    return plus(own, hop(left, axis, -1)) + hop(right, axis, 1).astype(jnp.float32)


def gather_across(v, axis):
    return [v, hop(v, axis, 1), hop(v, axis, -1), hop(v, axis, 2)]


def gather_before(v, axis):
    return [hop(v, axis, back) for back in (1, 2, 3)]


def send_back(parts, axis):
    return [hop(part, axis, -back) for back, part in zip((1, 2, 3), parts, strict=True)]


def gather_group(v, main, *early):
    column = gather_before(v[:main], "zlo")
    near = gather_across(v, "x")
    column, near, early = lax.optimization_barrier((column, near, early))
    far = gather_across(jnp.concatenate(column), "x")
    side = jnp.concatenate([part[main:] for part in near])
    return near, far + gather_before(side, "zlo"), early


def positions_of(rows, main):
    z, x, core = (lax.axis_index(a) for a in ("zlo", "x", "core"))
    n_z, n_x, n_core = (lax.axis_size(a) for a in ("zlo", "x", "core"))

    def at(back, over, start, stop):
        block = ((z + n_z - back) % n_z * n_x + (x + n_x + over) % n_x) * n_core + core
        return block * rows + jnp.arange(start, stop, dtype=jnp.int32)

    near = [at(0, over, 0, rows) for over in (0, -1, 1, 2)]
    far = [at(back, over, 0, main) for over in (0, -1, 1, 2) for back in (1, 2, 3)]
    side = [at(back, over, main, rows) for back in (1, 2, 3) for over in (0, -1, 1, 2)]
    return jnp.concatenate(near), jnp.concatenate(far + side)


def pieces_of(v, sizes):
    out, start = [], 0
    for size in sizes:
        out.append(v[start : start + size])
        start += size
    return out


def routed_experts(normed, ffn):
    ordered = lax.optimization_barrier
    bf16, f32 = jnp.bfloat16, jnp.float32
    rows = normed.shape[0]
    main = rows * 4 // 5 // 8 * 8
    cut = first_part(normed)

    def side_of(ring):
        return jnp.concatenate([ring[0][main:], ring[1][main:], ring[2][main:], ring[4][main - cut :]])

    column = gather_before(normed[:main], "zlo")
    near = gather_ring(normed, "x")
    column, near = ordered((column, near))
    column = jnp.concatenate(column)
    far_left, far_right = hop(column, "x", 1), hop(column, "x", -1)
    side = gather_before(side_of(near), "zlo")
    sizes = [v.shape[0] for v in near] + [column.shape[0]]
    first = ffn(jnp.concatenate(near + [column]))
    far_left, far_right, first = ordered((far_left, far_right, first))
    far_cut = first_part(column)
    far_low, far_high = hop(far_left[:far_cut], "x", 1), hop(far_right[far_cut:], "x", -1)
    second = ffn(jnp.concatenate([far_left, far_right]))
    far_low, far_high, side, second = ordered((far_low, far_high, side, second))
    last = ffn(jnp.concatenate([far_low, far_high] + side))

    *near, column = pieces_of(first, sizes)
    far_left, far_right = pieces_of(second, [column.shape[0]] * 2)
    far_low, far_high, *side = pieces_of(
        last, [far_low.shape[0], far_high.shape[0]] + [v.shape[0] for v in side]
    )
    low, high = hop(far_low, "x", -1), hop(far_high, "x", 1)
    side = send_back(side, "zlo")
    left = jnp.concatenate([plus(far_left[:far_cut], low).astype(bf16), far_left[far_cut:]])
    right = jnp.concatenate([far_right[:far_cut], plus(far_right[far_cut:], high).astype(bf16)])
    column = plus(column, hop(left, "x", -1)) + hop(right, "x", 1).astype(f32)
    column = send_back(pieces_of(column.astype(bf16), [main] * 3), "zlo")
    side, _ = ordered((side, (left, right)))
    side = plus(plus(side_of(near), side[0]), side[1]) + side[2].astype(f32)
    side = pieces_of(side.astype(bf16), [rows - main] * 4)
    near = [
        jnp.concatenate([near[0][:main], side[0]]),
        jnp.concatenate([near[1][:main], side[1]]),
        jnp.concatenate([near[2][:main], side[2]]),
        near[3],
        jnp.concatenate([near[4][: main - cut], side[3]]),
    ]
    near = reduce_ring(near, "x")
    top = plus(plus(near[:main], column[0]), column[1]) + column[2].astype(f32)
    return jnp.concatenate([top, near[main:]]).astype(bf16)


def local(
    hidden_in,
    query_vectors,
    key_vectors,
    value_vectors,
    out_weight,
    norm_gain,
    gate_proj,
    up_proj,
    down_proj,
    expert_ids,
    gate_scale,
):
    row_count, local_width = hidden_in.shape
    expert_count = lax.axis_size(EXP)
    block = lax.axis_index(CTX)
    capacity = min(row_count, 5 * row_count // (2 * expert_count))

    kv_main = row_count * 4 // 5 // 32 * 32
    near_pos, far_pos = positions_of(row_count, kv_main)
    across = (1 - 2 * lax.axis_index("core")) * row_count
    key_pos = jnp.concatenate([near_pos, near_pos + across, far_pos, far_pos + across])[None, :]
    query_pos = (block * row_count + jnp.arange(row_count, dtype=jnp.int32))[:, None]
    near, far, (key_pos, query_pos) = gather_group(
        jnp.concatenate([key_vectors, value_vectors], axis=1), kv_main, key_pos, query_pos
    )
    kv_near, kv_far = jnp.concatenate(near), jnp.concatenate(far)
    kv = [kv_near, lax.ppermute(kv_near, "core", SWAP), kv_far, lax.ppermute(kv_far, "core", SWAP)]

    experts = []
    for own in (gate_proj[0].T, up_proj[0].T, down_proj[0]):
        experts += [own, lax.ppermute(own, "core", SWAP)]

    flat_ids = expert_ids.reshape(row_count * 2)
    onehot = (
        flat_ids[:, None] == lax.broadcasted_iota(jnp.int32, (row_count * 2, expert_count), 1)
    ).astype(jnp.int32)
    earlier = jnp.cumsum(onehot, axis=0) - onehot
    slot_index = jnp.sum(earlier * onehot, axis=1)
    target = flat_ids * capacity + slot_index
    placing = (
        target[None, :]
        == lax.broadcasted_iota(jnp.int32, (expert_count * capacity, row_count * 2), 0)
    ).astype(jnp.bfloat16)
    placing_tokens = jnp.sum(placing.reshape(expert_count * capacity, row_count, 2), axis=2)

    zhi, y = lax.axis_index("zhi"), lax.axis_index("y")
    n_zhi, n_y = lax.axis_size("zhi"), lax.axis_size("y")
    order = jnp.stack(
        [
            (zhi + a) % n_zhi * n_y + (y + n_y + b) % n_y
            for b in (0, -1, 1, 2)
            for a in range(n_zhi)
        ]
    ).astype(jnp.int32)
    kv, experts = lax.optimization_barrier((kv, experts))
    own, left, right, far = attention(query_vectors, query_pos, key_pos, kv, out_weight, order)
    summed = plus(plus(own, hop(left, "y", -1)), hop(right, "y", 1)) + hop(far, "y", 2).astype(jnp.float32)
    mine, theirs = jnp.split(summed, 2, axis=1)
    projected = plus(mine, lax.ppermute(theirs.astype(jnp.bfloat16), "zhi", SWAP))
    residual = (hidden_in.astype(jnp.float32) + projected).astype(jnp.bfloat16)
    residual_wide = residual.astype(jnp.float32)

    buffer = jnp.dot(placing_tokens, residual, preferred_element_type=jnp.float32).astype(
        jnp.bfloat16
    )
    arrived = lax.all_to_all(buffer, EXP, split_axis=0, concat_axis=1, tiled=True)
    arrived_wide = arrived.astype(jnp.float32)
    inverse = lax.rsqrt(jnp.mean(arrived_wide * arrived_wide, axis=1, keepdims=True) + EPSILON)
    normed = (arrived_wide * inverse * norm_gain[None, :]).astype(jnp.bfloat16)

    result = routed_experts(normed, lambda rows: expert(rows, experts))

    returned = lax.all_to_all(result, EXP, split_axis=1, concat_axis=0, tiled=True)
    gathered_back = lax.dot_general(
        placing, returned, (((0,), (0,)), ((), ())), preferred_element_type=jnp.float32
    )
    gathered_back = gathered_back.reshape(row_count, 2, local_width)
    combined = (
        residual_wide
        + gate_scale[:, 0:1] * gathered_back[:, 0]
        + gate_scale[:, 1:2] * gathered_back[:, 1]
    )
    return combined.astype(jnp.bfloat16)


def solution(mesh):
    fine = Mesh(mesh.devices.reshape(4, 4, 2, 2, 4), AXES)
    placed = (
        P(CTX, EXP),
        P(CTX, EXP),
        P(CTX, EXP),
        P(CTX, EXP),
        P(EXP, None),
        P(),
        P(EXP, None, CTX),
        P(EXP, None, CTX),
        P(EXP, CTX, None),
        P(CTX, None),
        P(CTX, None),
    )
    return jax.shard_map(
        local, mesh=fine, in_specs=placed, out_specs=P(CTX, EXP), check_vma=False
    )
```

```python
import functools

import jax
import jax.numpy as jnp
from jax import lax
from jax.experimental import pallas as pl
from jax.experimental.pallas import tpu as pltpu
from jax.sharding import Mesh
from jax.sharding import PartitionSpec as P

HEAD_DIM = 128
EPSILON = 1e-05
MASKED = -1e30

AXES = ("zlo", "x", "core", "zhi", "y")
CTX = ("zlo", "x", "core")
RING = ("zlo", "x")
EXP = ("zhi", "y")
SWAP = [(0, 1), (1, 0)]

NT = (((1,), (1,)), ((), ()))


def attention_kernel(place_ref, query_ref, key_pos_ref, weight_ref, *refs, heads, chunk, pieces):
    kv_parts, out_refs, (kv_ref, scores_ref, attended_ref, sems) = (
        refs[:pieces],
        refs[pieces:-4],
        refs[-4:],
    )
    rows = query_ref.shape[0]
    copies, ends, end = [], [], 0
    for i, part in enumerate(kv_parts):
        copy = pltpu.make_async_copy(part, kv_ref.at[pl.ds(end, part.shape[0])], sems.at[i])
        copy.start()
        end += part.shape[0]
        copies.append(copy)
        ends.append(end)
    here = 0
    query_pos = place_ref[0] + lax.broadcasted_iota(jnp.int32, (rows, chunk), 0)
    for h in range(heads):
        cols = slice(h * HEAD_DIM, (h + 1) * HEAD_DIM)
        value_cols = slice((heads + h) * HEAD_DIM, (heads + h + 1) * HEAD_DIM)
        query = query_ref[:, cols]
        largest = jnp.full((rows, 128), MASKED, jnp.float32)
        for start in range(0, kv_ref.shape[0], chunk):
            at = slice(start, start + chunk)
            while here < pieces and (ends[here - 1] if here else 0) < start + chunk:
                copies[here].wait()
                here += 1
            scores = lax.dot_general(
                query, kv_ref[at, cols], NT, preferred_element_type=jnp.float32
            ) * HEAD_DIM ** (-0.5)
            scores = jnp.where(key_pos_ref[:, at] <= query_pos, scores, MASKED)
            scores_ref[:, at] = scores
            for lane in range(0, chunk, 128):
                largest = jnp.maximum(largest, scores[:, lane : lane + 128])
        largest = jnp.max(largest, axis=1, keepdims=True)
        total = jnp.zeros((rows, 128), jnp.float32)
        acc = jnp.zeros((rows, HEAD_DIM), jnp.float32)
        for start in range(0, kv_ref.shape[0], chunk):
            at = slice(start, start + chunk)
            weights = jnp.exp(scores_ref[:, at] - largest)
            for lane in range(0, chunk, 128):
                total = total + weights[:, lane : lane + 128]
            acc = acc + jnp.dot(
                weights.astype(jnp.bfloat16),
                kv_ref[at, value_cols],
                preferred_element_type=jnp.float32,
            )
        attended_ref[:, cols] = (acc / jnp.sum(total, axis=1, keepdims=True)).astype(
            attended_ref.dtype
        )
    blocks = place_ref.shape[0] - 1
    width = weight_ref.shape[1] // blocks
    per_out = blocks // len(out_refs)
    for j in range(blocks):
        start = pl.multiple_of(place_ref[1 + j] * width, width)
        out_ref, at = out_refs[j // per_out], j % per_out * width
        out_ref[:, at : at + width] = jnp.dot(
            attended_ref[...],
            weight_ref[:, pl.ds(start, width)],
            preferred_element_type=jnp.float32,
        ).astype(out_ref.dtype)


def attention(place, query, key_pos, kv, weight, chunk=512):
    rows, width = query.shape
    heads = width // HEAD_DIM
    keys = sum(part.shape[0] for part in kv)
    vmem = pl.BlockSpec(memory_space=pltpu.VMEM)
    return pl.pallas_call(
        functools.partial(attention_kernel, heads=heads, chunk=chunk, pieces=len(kv)),
        in_specs=[pl.BlockSpec(memory_space=pltpu.SMEM)]
        + [vmem] * 3
        + [pl.BlockSpec(memory_space=pltpu.HBM)] * len(kv),
        out_specs=[vmem] * 4,
        scratch_shapes=[
            pltpu.VMEM((keys, 2 * width), jnp.bfloat16),
            pltpu.VMEM((rows, keys), jnp.float32),
            pltpu.VMEM((rows, width), jnp.bfloat16),
            pltpu.SemaphoreType.DMA((len(kv),)),
        ],
        out_shape=[
            jax.ShapeDtypeStruct((rows, weight.shape[1] // 4), dtype)
            for dtype in (jnp.float32, jnp.bfloat16, jnp.bfloat16, jnp.bfloat16)
        ],
        cost_estimate=pl.CostEstimate(
            flops=4 * rows * width * keys + 2 * rows * weight.size,
            bytes_accessed=4 * keys * width,
            transcendentals=heads * rows * keys,
        ),
    )(place, query, key_pos, weight, *kv)


UNIT_TILE = 256


def expert_kernel(
    rows_ref, gate, gate_too, up, up_too, down, down_too, out_ref, w_in, w_down, hidden_ref, sems
):
    share = gate.shape[0]
    units = w_down.shape[0]
    half = units // 2
    copies = []
    for i, (source, target, start) in enumerate(
        [
            (gate, w_in, 0),
            (up, w_in, units),
            (gate_too, w_in, half),
            (up_too, w_in, units + half),
            (down, w_down, 0),
            (down_too, w_down, half),
        ]
    ):
        copy = pltpu.make_async_copy(source, target.at[pl.ds(start, share)], sems.at[i])
        copy.start()
        copies.append(copy)
    for target in (w_in, w_down):
        for start in range(0, target.shape[0], half):
            target[start + share : start + half] = jnp.zeros(
                (half - share, target.shape[1]), target.dtype
            )
    rows = rows_ref[...]
    ready = 0
    for start in range(0, units, UNIT_TILE):
        needed = 2 if start + UNIT_TILE <= half else 4
        while ready < needed:
            copies[ready].wait()
            ready += 1
        gate_act = lax.dot_general(
            rows, w_in[start : start + UNIT_TILE], NT, preferred_element_type=jnp.float32
        )
        up_act = lax.dot_general(
            rows,
            w_in[units + start : units + start + UNIT_TILE],
            NT,
            preferred_element_type=jnp.float32,
        )
        hidden_ref[:, start : start + UNIT_TILE] = (
            gate_act / (1.0 + jnp.exp(-gate_act)) * up_act
        ).astype(hidden_ref.dtype)
    for copy in copies[ready:]:
        copy.wait()
    hidden = hidden_ref[...]
    width = w_down.shape[1]
    for start in range(0, width, 512):
        out_ref[:, start : start + 512] = jnp.dot(
            hidden, w_down[:, start : start + 512], preferred_element_type=jnp.float32
        ).astype(out_ref.dtype)


def expert(rows, weights):
    count, width = rows.shape
    share = weights[0].shape[0]
    units = 2 * (-(-share // 128) * 128)
    return pl.pallas_call(
        expert_kernel,
        in_specs=[pl.BlockSpec(memory_space=pltpu.VMEM)]
        + [pl.BlockSpec(memory_space=pltpu.HBM)] * len(weights),
        out_specs=pl.BlockSpec(memory_space=pltpu.VMEM),
        scratch_shapes=[
            pltpu.VMEM((2 * units, width), jnp.bfloat16),
            pltpu.VMEM((units, width), jnp.bfloat16),
            pltpu.VMEM((count, units), jnp.bfloat16),
            pltpu.SemaphoreType.DMA((6,)),
        ],
        out_shape=jax.ShapeDtypeStruct((count, width), jnp.bfloat16),
        cost_estimate=pl.CostEstimate(
            flops=12 * count * width * share,
            bytes_accessed=12 * share * width,
            transcendentals=2 * count * share,
        ),
        compiler_params=pltpu.CompilerParams(vmem_limit_bytes=44 * 1024 * 1024),
    )(rows, *weights)


def joined_kernel(*refs):
    parts, out_ref, sems = refs[:-2], refs[-2], refs[-1]
    copies, end = [], 0
    for i, part in enumerate(parts):
        copies.append(
            pltpu.make_async_copy(part, out_ref.at[pl.ds(end, part.shape[0])], sems.at[i])
        )
        copies[-1].start()
        end += part.shape[0]
    for copy in copies:
        copy.wait()


def joined(parts):
    rows = sum(part.shape[0] for part in parts)
    return pl.pallas_call(
        joined_kernel,
        in_specs=[pl.BlockSpec(memory_space=pltpu.HBM)] * len(parts),
        out_specs=pl.BlockSpec(memory_space=pltpu.VMEM),
        scratch_shapes=[pltpu.SemaphoreType.DMA((len(parts),))],
        out_shape=jax.ShapeDtypeStruct((rows, parts[0].shape[1]), parts[0].dtype),
        cost_estimate=pl.CostEstimate(
            flops=0, bytes_accessed=4 * rows * parts[0].shape[1], transcendentals=0
        ),
    )(*parts)


def hop(v, axis, step):
    n = lax.axis_size(axis)
    return lax.ppermute(v, axis, [(i, (i + step) % n) for i in range(n)])


def first_part(v):
    return (v.shape[0] // 2 + 7) // 8 * 8


def plus(a, b):
    return a.astype(jnp.float32) + b.astype(jnp.float32)


def reduce_ring(parts, axis):
    own, left, right, far_low, far_high = parts
    cut = far_low.shape[0]
    low = hop(far_low.astype(jnp.bfloat16), axis, -1)
    high = hop(far_high.astype(jnp.bfloat16), axis, 1)
    left = jnp.concatenate([plus(left[:cut], low).astype(jnp.bfloat16), left[cut:].astype(jnp.bfloat16)])
    right = jnp.concatenate([right[:cut].astype(jnp.bfloat16), plus(right[cut:], high).astype(jnp.bfloat16)])
    return plus(own, hop(left, axis, -1)) + hop(right, axis, 1).astype(jnp.float32)


def gather_across(v, axis):
    return [v, hop(v, axis, 1), hop(v, axis, -1), hop(v, axis, 2)]


def reduce_across(parts, axis):
    own, left, right, far = parts
    near = plus(plus(own, hop(left, axis, -1)), hop(right, axis, 1))
    return near + hop(far, axis, 2).astype(jnp.float32)


def gather_before(v, axis):
    return [hop(v, axis, back) for back in (1, 2, 3)]


def send_back(parts, axis):
    return [hop(part, axis, -back) for back, part in zip((1, 2, 3), parts, strict=True)]


def gather_group(v, main, early):
    ordered = lax.optimization_barrier
    column = gather_before(v[:main], "zlo")
    near = gather_across(v, "x")
    near, early = ordered((near, early))
    side = jnp.concatenate([part[main:] for part in near])
    column, _ = ordered((column, near))
    far = gather_across(joined(column), "x")
    side = gather_before(side, "zlo")

    def other(part):
        return lax.ppermute(part, "core", SWAP)

    near_other, column_other = other(jnp.concatenate(near)), other(far[0])
    side_other = other(jnp.concatenate(side))
    kv = [*near, near_other, *column, *far[1:], *side, column_other, *map(other, far[1:]), side_other]
    return kv, early


def positions_of(rows, main):
    z, x, core = (lax.axis_index(a) for a in CTX)
    n_z, n_x, n_core = (lax.axis_size(a) for a in CTX)
    group = n_z * n_x * rows
    near, far = n_x * rows, (n_z - 1) * main
    j = jnp.arange(n_core * group, dtype=jnp.int32)
    is_near = j < n_core * near
    q = jnp.where(is_near, j % near, (j - n_core * near) % (group - near))
    across = jnp.where(is_near, j // near, (j - n_core * near) // (group - near))
    is_side = q >= n_x * far
    s = q - n_x * far
    rest = rows - main
    back = jnp.where(is_near, 0, 1 + jnp.where(is_side, s // (n_x * rest), q % far // main))
    row = jnp.where(is_near, q % rows, jnp.where(is_side, main + s % rest, q % main))
    over = jnp.where(is_near, q // rows, jnp.where(is_side, s % (n_x * rest) // rest, q // far))
    over = jnp.where(over == 1, -1, jnp.where(over > 1, over - 1, 0))
    block = ((z + n_z - back) % n_z * n_x + (x + n_x + over) % n_x) * n_core
    return (block + jnp.abs(core - across)) * rows + row


def pieces_of(v, sizes):
    out, start = [], 0
    for size in sizes:
        out.append(v[start : start + size])
        start += size
    return out


def routed_experts(normed, ffn):
    ordered = lax.optimization_barrier
    bf16, f32 = jnp.bfloat16, jnp.float32
    rows = normed.shape[0]
    main = rows * 4 // 5 // 8 * 8

    def side_of(ring):
        return jnp.concatenate([part[main:] for part in ring])

    def sizes(parts):
        return [part.shape[0] for part in parts]

    one, two, three = gather_before(normed[:main], "zlo")
    near = gather_across(normed, "x")
    one_left, one_right = hop(one, "x", 1), hop(one, "x", -1)
    near, _ = ordered((near, one))
    (two, three), (one_left, one_right) = ordered(((two, three), (one_left, one_right)))
    rest, around = ordered((jnp.concatenate([two, three]), side_of(near)))
    left, right = hop(rest, "x", 1), hop(rest, "x", -1)
    one_cut, cut = first_part(one), first_part(rest)
    one_low, one_high = hop(one_left[:one_cut], "x", 1), hop(one_right[one_cut:], "x", -1)
    side = gather_before(around, "zlo")
    first = near + [one, rest]
    first_out = ffn(jnp.concatenate(first))
    left, right, one_low, one_high, first_out = ordered((left, right, one_low, one_high, first_out))
    low, high = hop(left[:cut], "x", 1), hop(right[cut:], "x", -1)
    second = [one_left, one_right, one_low, one_high, left, right]
    second_out = ffn(jnp.concatenate(second))
    low, high, side, second_out = ordered((low, high, side, second_out))
    last = [low, high] + side
    last_out = ffn(jnp.concatenate(last))

    *near, one, rest = pieces_of(first_out, sizes(first))
    one_left, one_right, one_low, one_high, left, right = pieces_of(second_out, sizes(second))
    low, high, *side = pieces_of(last_out, sizes(last))
    one = reduce_ring([one, one_left, one_right, one_low, one_high], "x").astype(bf16)
    low, high = hop(low, "x", -1), hop(high, "x", 1)
    side = send_back(side, "zlo")
    left = jnp.concatenate([plus(left[:cut], low).astype(bf16), left[cut:]])
    right = jnp.concatenate([right[:cut], plus(right[cut:], high).astype(bf16)])
    rest = plus(rest, hop(left, "x", -1)) + hop(right, "x", 1).astype(f32)
    rest = rest.astype(bf16)
    column = send_back([one, rest[:main], rest[main:]], "zlo")
    side, _ = ordered((side, (left, right)))
    side = plus(plus(side_of(near), side[0]), side[1]) + side[2].astype(f32)
    side = pieces_of(side.astype(bf16), [rows - main] * 4)
    near = reduce_across(
        [jnp.concatenate([own[:main], rest]) for own, rest in zip(near, side, strict=True)], "x"
    )
    top = plus(plus(near[:main], column[0]), column[1]) + column[2].astype(f32)
    return jnp.concatenate([top, near[main:]]).astype(bf16)


def local(
    hidden_in,
    query_vectors,
    key_vectors,
    value_vectors,
    out_weight,
    norm_gain,
    gate_proj,
    up_proj,
    down_proj,
    expert_ids,
    gate_scale,
):
    row_count, local_width = hidden_in.shape
    expert_count = lax.axis_size(EXP)
    block = lax.axis_index(CTX)
    capacity = min(row_count, 5 * row_count // (2 * expert_count))

    kv_main = row_count * 4 // 5 // 32 * 32
    zhi = lax.axis_index("zhi")
    n_zhi, n_y = lax.axis_size("zhi"), lax.axis_size("y")
    y = lax.axis_index("y")
    place = jnp.stack(
        [block * row_count]
        + [
            (zhi + a) % n_zhi * n_y + (y + n_y + b) % n_y
            for b in (0, -1, 1, 2)
            for a in range(n_zhi)
        ]
    ).astype(jnp.int32)
    kv, (key_pos, place) = gather_group(
        jnp.concatenate([key_vectors, value_vectors], axis=1),
        kv_main,
        (positions_of(row_count, kv_main)[None, :], place),
    )

    experts = []
    for own in (gate_proj[0].T, up_proj[0].T, down_proj[0]):
        experts += [own, lax.ppermute(own, "core", SWAP)]

    flat_ids = expert_ids.reshape(row_count * 2)
    onehot = (
        flat_ids[:, None] == lax.broadcasted_iota(jnp.int32, (row_count * 2, expert_count), 1)
    ).astype(jnp.int32)
    earlier = jnp.cumsum(onehot, axis=0) - onehot
    slot_index = jnp.sum(earlier * onehot, axis=1)
    target = flat_ids * capacity + slot_index
    placing = (
        target[None, :]
        == lax.broadcasted_iota(jnp.int32, (expert_count * capacity, row_count * 2), 0)
    ).astype(jnp.bfloat16)
    placing_tokens = jnp.sum(placing.reshape(expert_count * capacity, row_count, 2), axis=2)

    kv, experts = lax.optimization_barrier((kv, experts))
    own, left, right, far = attention(place, query_vectors, key_pos, kv, out_weight)
    summed = plus(plus(own, hop(left, "y", -1)), hop(right, "y", 1)) + hop(far, "y", 2).astype(jnp.float32)
    mine, theirs = jnp.split(summed, 2, axis=1)
    projected = plus(mine, lax.ppermute(theirs.astype(jnp.bfloat16), "zhi", SWAP))
    residual = (hidden_in.astype(jnp.float32) + projected).astype(jnp.bfloat16)
    residual_wide = residual.astype(jnp.float32)

    buffer = jnp.dot(placing_tokens, residual, preferred_element_type=jnp.float32).astype(
        jnp.bfloat16
    )
    arrived = lax.all_to_all(buffer, EXP, split_axis=0, concat_axis=1, tiled=True)
    arrived_wide = arrived.astype(jnp.float32)
    inverse = lax.rsqrt(jnp.mean(arrived_wide * arrived_wide, axis=1, keepdims=True) + EPSILON)
    normed = (arrived_wide * inverse * norm_gain[None, :]).astype(jnp.bfloat16)

    result = routed_experts(normed, lambda rows: expert(rows, experts))

    returned = lax.all_to_all(result, EXP, split_axis=1, concat_axis=0, tiled=True)
    gathered_back = lax.dot_general(
        placing, returned, (((0,), (0,)), ((), ())), preferred_element_type=jnp.float32
    )
    gathered_back = gathered_back.reshape(row_count, 2, local_width)
    combined = (
        residual_wide
        + gate_scale[:, 0:1] * gathered_back[:, 0]
        + gate_scale[:, 1:2] * gathered_back[:, 1]
    )
    return combined.astype(jnp.bfloat16)


def solution(mesh):
    fine = Mesh(mesh.devices.reshape(4, 4, 2, 2, 4), AXES)
    placed = (
        P(CTX, EXP),
        P(CTX, EXP),
        P(CTX, EXP),
        P(CTX, EXP),
        P(EXP, None),
        P(),
        P(EXP, None, CTX),
        P(EXP, None, CTX),
        P(EXP, CTX, None),
        P(CTX, None),
        P(CTX, None),
    )
    return jax.shard_map(
        local, mesh=fine, in_specs=placed, out_specs=P(CTX, EXP), check_vma=False
    )
```

```python
import functools

import jax
import jax.numpy as jnp
from jax import lax
from jax.experimental import pallas as pl
from jax.experimental.pallas import tpu as pltpu
from jax.sharding import Mesh
from jax.sharding import PartitionSpec as P

HEAD_DIM = 128
EPSILON = 1e-05
MASKED = -1e30

AXES = ("zlo", "x", "core", "zhi", "y")
CTX = ("zlo", "x", "core")
RING = ("zlo", "x")
EXP = ("zhi", "y")
SWAP = [(0, 1), (1, 0)]

NT = (((1,), (1,)), ((), ()))


def attention_kernel(place_ref, query_ref, key_pos_ref, weight_ref, *refs, heads, chunk, pieces):
    kv_parts, out_refs, (kv_ref, scores_ref, attended_ref, sems) = (
        refs[:pieces],
        refs[pieces:-4],
        refs[-4:],
    )
    rows = query_ref.shape[0]
    copies, ends, end = [], [], 0
    for i, part in enumerate(kv_parts):
        copy = pltpu.make_async_copy(part, kv_ref.at[pl.ds(end, part.shape[0])], sems.at[i])
        copy.start()
        end += part.shape[0]
        copies.append(copy)
        ends.append(end)
    here = 0
    query_pos = place_ref[0] + lax.broadcasted_iota(jnp.int32, (rows, chunk), 0)
    for h in range(heads):
        cols = slice(h * HEAD_DIM, (h + 1) * HEAD_DIM)
        value_cols = slice((heads + h) * HEAD_DIM, (heads + h + 1) * HEAD_DIM)
        query = query_ref[:, cols]
        largest = jnp.full((rows, 128), MASKED, jnp.float32)
        for start in range(0, kv_ref.shape[0], chunk):
            at = slice(start, start + chunk)
            while here < pieces and (ends[here - 1] if here else 0) < start + chunk:
                copies[here].wait()
                here += 1
            scores = lax.dot_general(
                query, kv_ref[at, cols], NT, preferred_element_type=jnp.float32
            ) * HEAD_DIM ** (-0.5)
            scores = jnp.where(key_pos_ref[:, at] <= query_pos, scores, MASKED)
            scores_ref[:, at] = scores
            for lane in range(0, chunk, 128):
                largest = jnp.maximum(largest, scores[:, lane : lane + 128])
        largest = jnp.max(largest, axis=1, keepdims=True)
        total = jnp.zeros((rows, 128), jnp.float32)
        acc = jnp.zeros((rows, HEAD_DIM), jnp.float32)
        for start in range(0, kv_ref.shape[0], chunk):
            at = slice(start, start + chunk)
            weights = jnp.exp(scores_ref[:, at] - largest)
            for lane in range(0, chunk, 128):
                total = total + weights[:, lane : lane + 128]
            acc = acc + jnp.dot(
                weights.astype(jnp.bfloat16),
                kv_ref[at, value_cols],
                preferred_element_type=jnp.float32,
            )
        attended_ref[:, cols] = (acc / jnp.sum(total, axis=1, keepdims=True)).astype(
            attended_ref.dtype
        )
    blocks = place_ref.shape[0] - 1
    width = weight_ref.shape[1] // blocks
    per_out = blocks // len(out_refs)
    for j in range(blocks):
        start = pl.multiple_of(place_ref[1 + j] * width, width)
        out_ref, at = out_refs[j // per_out], j % per_out * width
        out_ref[:, at : at + width] = jnp.dot(
            attended_ref[...],
            weight_ref[:, pl.ds(start, width)],
            preferred_element_type=jnp.float32,
        ).astype(out_ref.dtype)


def attention(place, query, key_pos, kv, weight, chunk=512):
    rows, width = query.shape
    heads = width // HEAD_DIM
    keys = sum(part.shape[0] for part in kv)
    vmem = pl.BlockSpec(memory_space=pltpu.VMEM)
    return pl.pallas_call(
        functools.partial(attention_kernel, heads=heads, chunk=chunk, pieces=len(kv)),
        in_specs=[pl.BlockSpec(memory_space=pltpu.SMEM)]
        + [vmem] * 3
        + [pl.BlockSpec(memory_space=pltpu.HBM)] * len(kv),
        out_specs=[vmem] * 4,
        scratch_shapes=[
            pltpu.VMEM((keys, 2 * width), jnp.bfloat16),
            pltpu.VMEM((rows, keys), jnp.float32),
            pltpu.VMEM((rows, width), jnp.bfloat16),
            pltpu.SemaphoreType.DMA((len(kv),)),
        ],
        out_shape=[
            jax.ShapeDtypeStruct((rows, weight.shape[1] // 4), dtype)
            for dtype in (jnp.float32, jnp.bfloat16, jnp.bfloat16, jnp.bfloat16)
        ],
        cost_estimate=pl.CostEstimate(
            flops=4 * rows * width * keys + 2 * rows * weight.size,
            bytes_accessed=4 * keys * width,
            transcendentals=heads * rows * keys,
        ),
    )(place, query, key_pos, weight, *kv)


UNIT_TILE = 256


def expert_kernel(
    rows_ref, gate, gate_too, up, up_too, down, down_too, out_ref, w_in, w_down, hidden_ref, sems
):
    share = gate.shape[0]
    units = w_down.shape[0]
    half = units // 2
    copies = []
    for i, (source, target, start) in enumerate(
        [
            (gate, w_in, 0),
            (up, w_in, units),
            (gate_too, w_in, half),
            (up_too, w_in, units + half),
            (down, w_down, 0),
            (down_too, w_down, half),
        ]
    ):
        copy = pltpu.make_async_copy(source, target.at[pl.ds(start, share)], sems.at[i])
        copy.start()
        copies.append(copy)
    for target in (w_in, w_down):
        for start in range(0, target.shape[0], half):
            target[start + share : start + half] = jnp.zeros(
                (half - share, target.shape[1]), target.dtype
            )
    rows = rows_ref[...]
    ready = 0
    for start in range(0, units, UNIT_TILE):
        needed = 2 if start + UNIT_TILE <= half else 4
        while ready < needed:
            copies[ready].wait()
            ready += 1
        gate_act = lax.dot_general(
            rows, w_in[start : start + UNIT_TILE], NT, preferred_element_type=jnp.float32
        )
        up_act = lax.dot_general(
            rows,
            w_in[units + start : units + start + UNIT_TILE],
            NT,
            preferred_element_type=jnp.float32,
        )
        hidden_ref[:, start : start + UNIT_TILE] = (
            gate_act / (1.0 + jnp.exp(-gate_act)) * up_act
        ).astype(hidden_ref.dtype)
    for copy in copies[ready:]:
        copy.wait()
    hidden = hidden_ref[...]
    width = w_down.shape[1]
    for start in range(0, width, 512):
        out_ref[:, start : start + 512] = jnp.dot(
            hidden, w_down[:, start : start + 512], preferred_element_type=jnp.float32
        ).astype(out_ref.dtype)


def expert(rows, weights):
    count, width = rows.shape
    share = weights[0].shape[0]
    units = 2 * (-(-share // 128) * 128)
    return pl.pallas_call(
        expert_kernel,
        in_specs=[pl.BlockSpec(memory_space=pltpu.VMEM)]
        + [pl.BlockSpec(memory_space=pltpu.HBM)] * len(weights),
        out_specs=pl.BlockSpec(memory_space=pltpu.VMEM),
        scratch_shapes=[
            pltpu.VMEM((2 * units, width), jnp.bfloat16),
            pltpu.VMEM((units, width), jnp.bfloat16),
            pltpu.VMEM((count, units), jnp.bfloat16),
            pltpu.SemaphoreType.DMA((6,)),
        ],
        out_shape=jax.ShapeDtypeStruct((count, width), jnp.bfloat16),
        cost_estimate=pl.CostEstimate(
            flops=12 * count * width * share,
            bytes_accessed=12 * share * width,
            transcendentals=2 * count * share,
        ),
        compiler_params=pltpu.CompilerParams(vmem_limit_bytes=44 * 1024 * 1024),
    )(rows, *weights)


def joined_kernel(*refs):
    parts, out_ref, sems = refs[:-2], refs[-2], refs[-1]
    copies, end = [], 0
    for i, part in enumerate(parts):
        copies.append(
            pltpu.make_async_copy(part, out_ref.at[pl.ds(end, part.shape[0])], sems.at[i])
        )
        copies[-1].start()
        end += part.shape[0]
    for copy in copies:
        copy.wait()


def joined(parts):
    rows = sum(part.shape[0] for part in parts)
    return pl.pallas_call(
        joined_kernel,
        in_specs=[pl.BlockSpec(memory_space=pltpu.HBM)] * len(parts),
        out_specs=pl.BlockSpec(memory_space=pltpu.VMEM),
        scratch_shapes=[pltpu.SemaphoreType.DMA((len(parts),))],
        out_shape=jax.ShapeDtypeStruct((rows, parts[0].shape[1]), parts[0].dtype),
        cost_estimate=pl.CostEstimate(
            flops=0, bytes_accessed=4 * rows * parts[0].shape[1], transcendentals=0
        ),
    )(*parts)


def hop(v, axis, step):
    n = lax.axis_size(axis)
    return lax.ppermute(v, axis, [(i, (i + step) % n) for i in range(n)])


def first_part(v):
    return (v.shape[0] // 2 + 7) // 8 * 8


def plus(a, b):
    return a.astype(jnp.float32) + b.astype(jnp.float32)


def reduce_ring(parts, axis):
    own, left, right, far_low, far_high = parts
    cut = far_low.shape[0]
    low = hop(far_low.astype(jnp.bfloat16), axis, -1)
    high = hop(far_high.astype(jnp.bfloat16), axis, 1)
    left = jnp.concatenate([plus(left[:cut], low).astype(jnp.bfloat16), left[cut:].astype(jnp.bfloat16)])
    right = jnp.concatenate([right[:cut].astype(jnp.bfloat16), plus(right[cut:], high).astype(jnp.bfloat16)])
    return plus(own, hop(left, axis, -1)) + hop(right, axis, 1).astype(jnp.float32)


def gather_across(v, axis):
    return [v, hop(v, axis, 1), hop(v, axis, -1), hop(v, axis, 2)]


def reduce_across(parts, axis):
    own, left, right, far = parts
    near = plus(plus(own, hop(left, axis, -1)), hop(right, axis, 1))
    return near + hop(far, axis, 2).astype(jnp.float32)


def gather_before(v, axis):
    return [hop(v, axis, back) for back in (1, 2, 3)]


def send_back(parts, axis):
    return [hop(part, axis, -back) for back, part in zip((1, 2, 3), parts, strict=True)]


def gather_group(v, main, early):
    ordered = lax.optimization_barrier
    column = gather_before(v[:main], "zlo")
    near = gather_across(v, "x")
    near, early = ordered((near, early))
    side = jnp.concatenate([part[main:] for part in near])
    column, _ = ordered((column, near))
    far = gather_across(joined(column), "x")
    side = gather_before(side, "zlo")

    def other(part):
        return lax.ppermute(part, "core", SWAP)

    near_other, column_other = other(jnp.concatenate(near)), other(far[0])
    side_other = other(jnp.concatenate(side))
    kv = [*near, near_other, *column, *far[1:], *side, column_other, *map(other, far[1:]), side_other]
    return kv, early


def positions_of(rows, main):
    z, x, core = (lax.axis_index(a) for a in CTX)
    n_z, n_x, n_core = (lax.axis_size(a) for a in CTX)
    group = n_z * n_x * rows
    near, far = n_x * rows, (n_z - 1) * main
    j = jnp.arange(n_core * group, dtype=jnp.int32)
    is_near = j < n_core * near
    q = jnp.where(is_near, j % near, (j - n_core * near) % (group - near))
    across = jnp.where(is_near, j // near, (j - n_core * near) // (group - near))
    is_side = q >= n_x * far
    s = q - n_x * far
    rest = rows - main
    back = jnp.where(is_near, 0, 1 + jnp.where(is_side, s // (n_x * rest), q % far // main))
    row = jnp.where(is_near, q % rows, jnp.where(is_side, main + s % rest, q % main))
    over = jnp.where(is_near, q // rows, jnp.where(is_side, s % (n_x * rest) // rest, q // far))
    over = jnp.where(over == 1, -1, jnp.where(over > 1, over - 1, 0))
    block = ((z + n_z - back) % n_z * n_x + (x + n_x + over) % n_x) * n_core
    return (block + jnp.abs(core - across)) * rows + row


def pieces_of(v, sizes):
    out, start = [], 0
    for size in sizes:
        out.append(v[start : start + size])
        start += size
    return out


def routed_experts(normed, ffn):
    ordered = lax.optimization_barrier
    bf16, f32 = jnp.bfloat16, jnp.float32
    rows = normed.shape[0]
    main = rows * 4 // 5 // 8 * 8

    def side_of(ring):
        return jnp.concatenate([part[main:] for part in ring])

    def sizes(parts):
        return [part.shape[0] for part in parts]

    one, two, three = gather_before(normed[:main], "zlo")
    near = gather_across(normed, "x")
    one_left, one_right = hop(one, "x", 1), hop(one, "x", -1)
    near, _ = ordered((near, one))
    (two, three), (one_left, one_right) = ordered(((two, three), (one_left, one_right)))
    rest, around = ordered((jnp.concatenate([two, three]), side_of(near)))
    left, right = hop(rest, "x", 1), hop(rest, "x", -1)
    one_cut, cut = first_part(one), first_part(rest)
    one_low, one_high = hop(one_left[:one_cut], "x", 1), hop(one_right[one_cut:], "x", -1)
    side = gather_before(around, "zlo")
    first = near + [one, rest]
    first_out = ffn(jnp.concatenate(first))
    low, high = hop(left[:cut], "x", 1), hop(right[cut:], "x", -1)
    second = [one_left, one_right, one_low, one_high, left, right]
    second_out = ffn(jnp.concatenate(second))
    low, high, side, second_out = ordered((low, high, side, second_out))
    last = [low, high] + side
    last_out = ffn(jnp.concatenate(last))

    *near, one, rest = pieces_of(first_out, sizes(first))
    one_left, one_right, one_low, one_high, left, right = pieces_of(second_out, sizes(second))
    low, high, *side = pieces_of(last_out, sizes(last))
    one = reduce_ring([one, one_left, one_right, one_low, one_high], "x").astype(bf16)
    low, high = hop(low, "x", -1), hop(high, "x", 1)
    side = send_back(side, "zlo")
    left = jnp.concatenate([plus(left[:cut], low).astype(bf16), left[cut:]])
    right = jnp.concatenate([right[:cut], plus(right[cut:], high).astype(bf16)])
    rest = plus(rest, hop(left, "x", -1)) + hop(right, "x", 1).astype(f32)
    rest = rest.astype(bf16)
    column = send_back([one, rest[:main], rest[main:]], "zlo")
    side, _ = ordered((side, (left, right)))
    side = plus(plus(side_of(near), side[0]), side[1]) + side[2].astype(f32)
    side = pieces_of(side.astype(bf16), [rows - main] * 4)
    near = reduce_across(
        [jnp.concatenate([own[:main], rest]) for own, rest in zip(near, side, strict=True)], "x"
    )
    top = plus(plus(near[:main], column[0]), column[1]) + column[2].astype(f32)
    return jnp.concatenate([top, near[main:]]).astype(bf16)


def local(
    hidden_in,
    query_vectors,
    key_vectors,
    value_vectors,
    out_weight,
    norm_gain,
    gate_proj,
    up_proj,
    down_proj,
    expert_ids,
    gate_scale,
):
    row_count, local_width = hidden_in.shape
    expert_count = lax.axis_size(EXP)
    block = lax.axis_index(CTX)
    capacity = min(row_count, 5 * row_count // (2 * expert_count))

    kv_main = row_count * 4 // 5 // 32 * 32
    zhi = lax.axis_index("zhi")
    n_zhi, n_y = lax.axis_size("zhi"), lax.axis_size("y")
    y = lax.axis_index("y")
    place = jnp.stack(
        [block * row_count]
        + [
            (zhi + a) % n_zhi * n_y + (y + n_y + b) % n_y
            for b in (0, -1, 1, 2)
            for a in range(n_zhi)
        ]
    ).astype(jnp.int32)
    kv, (key_pos, place) = gather_group(
        jnp.concatenate([key_vectors, value_vectors], axis=1),
        kv_main,
        (positions_of(row_count, kv_main)[None, :], place),
    )

    experts = []
    for own in (gate_proj[0].T, up_proj[0].T, down_proj[0]):
        experts += [own, lax.ppermute(own, "core", SWAP)]

    flat_ids = expert_ids.reshape(row_count * 2)
    onehot = (
        flat_ids[:, None] == lax.broadcasted_iota(jnp.int32, (row_count * 2, expert_count), 1)
    ).astype(jnp.int32)
    earlier = jnp.cumsum(onehot, axis=0) - onehot
    slot_index = jnp.sum(earlier * onehot, axis=1)
    target = flat_ids * capacity + slot_index
    placing = (
        target[None, :]
        == lax.broadcasted_iota(jnp.int32, (expert_count * capacity, row_count * 2), 0)
    ).astype(jnp.bfloat16)
    placing_tokens = jnp.sum(placing.reshape(expert_count * capacity, row_count, 2), axis=2)

    kv, experts = lax.optimization_barrier((kv, experts))
    own, left, right, far = attention(place, query_vectors, key_pos, kv, out_weight)
    summed = plus(plus(own, hop(left, "y", -1)), hop(right, "y", 1)) + hop(far, "y", 2).astype(jnp.float32)
    mine, theirs = jnp.split(summed, 2, axis=1)
    projected = plus(mine, lax.ppermute(theirs.astype(jnp.bfloat16), "zhi", SWAP))
    residual = (hidden_in.astype(jnp.float32) + projected).astype(jnp.bfloat16)
    residual_wide = residual.astype(jnp.float32)

    buffer = jnp.dot(placing_tokens, residual, preferred_element_type=jnp.float32).astype(
        jnp.bfloat16
    )
    arrived = lax.all_to_all(buffer, EXP, split_axis=0, concat_axis=1, tiled=True)
    arrived_wide = arrived.astype(jnp.float32)
    inverse = lax.rsqrt(jnp.mean(arrived_wide * arrived_wide, axis=1, keepdims=True) + EPSILON)
    normed = (arrived_wide * inverse * norm_gain[None, :]).astype(jnp.bfloat16)

    result = routed_experts(normed, lambda rows: expert(rows, experts))

    returned = lax.all_to_all(result, EXP, split_axis=1, concat_axis=0, tiled=True)
    gathered_back = lax.dot_general(
        placing, returned, (((0,), (0,)), ((), ())), preferred_element_type=jnp.float32
    )
    gathered_back = gathered_back.reshape(row_count, 2, local_width)
    combined = (
        residual_wide
        + gate_scale[:, 0:1] * gathered_back[:, 0]
        + gate_scale[:, 1:2] * gathered_back[:, 1]
    )
    return combined.astype(jnp.bfloat16)


def solution(mesh):
    fine = Mesh(mesh.devices.reshape(4, 4, 2, 2, 4), AXES)
    placed = (
        P(CTX, EXP),
        P(CTX, EXP),
        P(CTX, EXP),
        P(CTX, EXP),
        P(EXP, None),
        P(),
        P(EXP, None, CTX),
        P(EXP, None, CTX),
        P(EXP, CTX, None),
        P(CTX, None),
        P(CTX, None),
    )
    return jax.shard_map(
        local, mesh=fine, in_specs=placed, out_specs=P(CTX, EXP), check_vma=False
    )
```
